32 devices in a mesh: gx: 4 (over z), gy: 2 (over y), gz: 4 (over x, core).
Axes of the slice: x: 2, y: 2, z: 4, core: 2. Of those that a mesh axis runs over, the one named last changes fastest.
Arguments:
- positions: float32 [3, 16, 8, 8, 128], P(None, 'gx', 'gy', 'gz'), may hold values from 0 to 1
- line_vectors: float32 [3, 16, 8, 8, 128], P(None, 'gx', 'gy', 'gz'), may hold values from -3 to 3
- burgers: float32 [3, 16, 8, 8, 128], P(None, 'gx', 'gy', 'gz'), may hold values from -6 to 6
- mobility: float32 [16, 8, 8, 128], P('gx', 'gy', 'gz'), may hold values from 0.25 to 4
- occupancy: int32 [16, 8, 8], P('gx', 'gy', 'gz'), may hold values from 1 to 128
Outputs:
- moved_positions: float32 [3, 16, 8, 8, 128], P(None, 'gx', 'gy', 'gz')
- end_forces: float32 [3, 16, 8, 8, 128], P(None, 'gx', 'gy', 'gz')
The draws below stay inside these ranges and needn't reach their ends.
All inputs are finite; a program needn't handle non-finite values.
Results may differ from the reference program's by a relative error of at most 0.0001.
Values sent between devices are 32-bit elements; how exact they have to be, the bound alone decides.
A program may use at most 64 MiB of HBM per device.

```python
import math
import jax
import jax.numpy as jnp
from jax import lax

SLOTS = 128
NCX = 16
NCY = 8
NCZ = 8


def place_ends(values, own_key, least, largest):
    dims = values.shape
    spot = [jax.random.randint(jax.random.fold_in(own_key, axis), (), 0, dims[axis]) for axis in range(len(dims))]
    values = values.at[tuple(spot)].set(least)
    longest = dims.index(max(dims))
    spot[longest] = (spot[longest] + 1) % dims[longest]
    return values.at[tuple(spot)].set(largest)


def steps_of(stream_key, shape, cuts, smallest, largest):
    def one(axis_at, blocks):
        steps = jax.random.uniform(jax.random.fold_in(jax.random.fold_in(stream_key, 6), axis_at), (blocks,), jnp.float32, smallest / len(cuts), largest / len(cuts))
        return jnp.repeat(jnp.exp(steps), shape[axis_at] // blocks).reshape((-1,) + (1,) * (len(shape) - axis_at - 1))

    level = one(*cuts[0])
    for cut in cuts[1:]:
        level = level * one(*cut)
    return level


def scatter_about(own_key, shape, scale, most, cuts=(), dtype=jnp.bfloat16):
    factor_of = steps_of(own_key, shape, cuts, -0.22, 0.18) if cuts else 1.0
    drawn = jax.random.normal(own_key, shape, jnp.float32) * scale * factor_of
    return jnp.minimum(jnp.maximum(drawn, -most), most).astype(dtype)


def setup_inputs(seed: int = 0) -> dict:
    arg_keys = jax.random.split(jax.random.key(seed), 6)
    return {
        "positions": jnp.clip(1.0 * jax.random.uniform(arg_keys[0], (3, NCX, NCY, NCZ, SLOTS), jnp.float32) ** steps_of(arg_keys[0], (3, NCX, NCY, NCZ, SLOTS), ((1, 4), (2, 2), (3, 4)), -0.2, 0.2), 0.0, 1.0),
        "line_vectors": scatter_about(arg_keys[1], (3, NCX, NCY, NCZ, SLOTS), 0.5, 3.0, ((1, 4), (2, 2), (3, 4)), jnp.float32),
        "burgers": scatter_about(arg_keys[2], (3, NCX, NCY, NCZ, SLOTS), 1.0, 6.0, ((1, 4), (2, 2), (3, 4)), jnp.float32),
        "mobility": jnp.clip(jnp.exp(math.log(4.0) - 2.7725887 * jax.random.uniform(arg_keys[3], (NCX, NCY, NCZ, SLOTS), jnp.float32) ** steps_of(arg_keys[3], (NCX, NCY, NCZ, SLOTS), ((0, 4), (1, 2), (2, 4)), -0.2, 0.2)), 0.25, 4.0),
        "occupancy": place_ends(jax.random.randint(arg_keys[4], (NCX, NCY, NCZ), 1, SLOTS + 1), jax.random.fold_in(arg_keys[4], 1), 1, SLOTS).astype(jnp.int32),
    }


CORE_SQUARED = 0.25
MU_SCALE = 0.05
CROSS_WEIGHT = 0.5
STEP_LIMIT = 0.1
NEIGHBOUR_SHIFTS = [(first, second, third) for first in (-1, 0, 1) for second in (-1, 0, 1) for third in (-1, 0, 1)]

def inner_pairs(left, right):
    return sum((left[k][..., :, None] * right[k][..., None, :] for k in range(3)))

def tile_force(target, source, offset):
    separate = [target[k][..., :, None] - source[k][..., None, :] - float(offset[k]) for k in range(3)]
    radius_sq = separate[0] * separate[0] + separate[1] * separate[1] + separate[2] * separate[2] + CORE_SQUARED
    inverse = lax.rsqrt(radius_sq)
    couple = inner_pairs(target[6:9], source[6:9]) * inner_pairs(target[3:6], source[3:6])
    couple = couple - CROSS_WEIGHT * inner_pairs(target[6:9], source[3:6]) * inner_pairs(target[3:6], source[6:9])
    weight = couple * source[9][..., None, :] * inverse * inverse * inverse
    return jnp.stack([lax.optimization_barrier(jnp.sum(weight * separate[k], axis=-1)) for k in range(3)]) * (MU_SCALE * target[9])

def all_forces(fields):
    total = jnp.zeros((3,) + fields.shape[1:], jnp.float32)
    for offset in NEIGHBOUR_SHIFTS:
        source = jnp.roll(fields, (-offset[0], -offset[1], -offset[2]), (1, 2, 3))
        both = jnp.moveaxis(jnp.stack([fields, source]), 2, 0)
        slabs = lax.map(lambda pair: tile_force(pair[0], pair[1], offset), both)
        total = total + jnp.moveaxis(slabs, 0, 1)
    return total

def reference(positions, line_vectors, burgers, mobility, occupancy):
    slots = lax.broadcasted_iota(jnp.int32, mobility.shape, 3)
    live = (slots < occupancy[..., None]).astype(jnp.float32)
    fixed_part = jnp.concatenate([line_vectors, burgers, live[None]], 0)
    start_forces = all_forces(jnp.concatenate([positions, fixed_part], 0))
    speed0 = mobility[None] * start_forces
    peak = jnp.max(lax.optimization_barrier(jnp.sum(speed0 * speed0, axis=0)))
    step = STEP_LIMIT * lax.rsqrt(peak + 1e-12)
    predicted = positions + step * speed0
    end_forces = all_forces(jnp.concatenate([predicted, fixed_part], 0))
    moved_positions = positions + 0.5 * step * (speed0 + mobility[None] * end_forces)
    return (moved_positions, end_forces)
```

```python
import functools

import jax
import jax.numpy as jnp
from jax import lax
from jax.experimental import pallas as pl
from jax.experimental.pallas import tpu as pltpu
from jax.sharding import PartitionSpec as P

CORE_SQUARED = 0.25
MU_SCALE = 0.05
CROSS_WEIGHT = 0.5
STEP_LIMIT = 0.1
AXES = ("gx", "gy", "gz")
K_ROWS = 72


def extended(block):
    for dim, axis in enumerate(AXES):
        count = lax.axis_size(axis)
        forward = [(i, (i + 1) % count) for i in range(count)]
        backward = [(target, source) for source, target in forward]
        low = lax.ppermute(
            lax.slice_in_dim(block, block.shape[dim] - 1, None, axis=dim), axis, forward
        )
        high = lax.ppermute(lax.slice_in_dim(block, 0, 1, axis=dim), axis, backward)
        block = jnp.concatenate([low, block, high], axis=dim)
    return block


def split(value, parts):
    terms = []
    for _ in range(parts):
        term = value.astype(jnp.bfloat16).astype(jnp.float32)
        terms.append(term)
        value = value - term
    return terms


def offsets(row, index, local):
    corner = [i.astype(jnp.float32) - (1.0 + n / 2) for i, n in zip(index, local)]
    return jnp.where(row == 0, corner[0], jnp.where(row == 1, corner[1], corner[2]))


def source_rows(fix, place, row):
    live = fix[3:4]
    turned = pltpu.roll(fix, 4, 0)
    keep = jnp.where(row < 3, live, 0.0)
    lines, burgers = fix * keep, turned * keep
    high, low = [], []
    for a in range(3):
        form = fix[4 + a : 5 + a] * lines - CROSS_WEIGHT * fix[a : a + 1] * burgers
        first, second = split(form, 2)
        high.append(first)
        low.append(second)
    square = jnp.sum(place * place, axis=0, keepdims=True) + CORE_SQUARED
    vec = jnp.where(row < 3, place, jnp.where(row == 3, square, jnp.where(row == 4, 1.0, 0.0)))
    h, m, l = split(vec, 3)
    zero = jnp.zeros_like(h)
    return jnp.concatenate(high + low + high + [h, m, h, m, l, h, zero], axis=0)


def target_rows(fix, place, row):
    high, low = [], []
    for a in range(3):
        first, second = split(fix[4 + a : 5 + a] * fix, 2)
        high.append(first)
        low.append(second)
    square = jnp.sum(place * place, axis=0, keepdims=True)
    vec = jnp.where(
        row < 3, -2.0 * place, jnp.where(row == 3, 1.0, jnp.where(row == 4, square, 0.0))
    )
    h, m, l = split(vec, 3)
    zero = jnp.zeros_like(h)
    return jnp.concatenate(high + high + low + [h, h, m, m, h, l, zero], axis=0)


def sweep(local, slots, occ_ref, fix_ref, pos_ref, base_ref, place_ref, lhs_ref, acc_ref, emit):
    ext = tuple(n + 2 for n in local)
    row = lax.broadcasted_iota(jnp.int32, (8, slots), 0)

    def prepare(c, carry):
        z = lax.rem(c, ext[2])
        y = lax.rem(c // ext[2], ext[1])
        x = c // (ext[2] * ext[1])
        place = jnp.where(row < 3, pos_ref[x, y, z] + offsets(row, (x, y, z), local), 0.0)
        place_ref[x, y, z] = place
        base_ref[x, y, z] = source_rows(fix_ref[x, y, z], place, row).astype(jnp.bfloat16)
        return carry

    lax.fori_loop(0, ext[0] * ext[1] * ext[2], prepare, 0)

    def one_cell(c, carry):
        z = lax.rem(c, local[2])
        y = lax.rem(c // local[2], local[1])
        x = c // (local[2] * local[1])
        fix = fix_ref[x + 1, y + 1, z + 1]
        place = place_ref[x + 1, y + 1, z + 1]
        turned = target_rows(fix, place, row).T
        lane = lax.broadcasted_iota(jnp.int32, turned.shape, 1)
        lhs_ref[0] = jnp.where(lane < K_ROWS, turned, 0.0).astype(jnp.bfloat16)
        lhs_ref[1] = jnp.where(lane < K_ROWS, 0.0, turned).astype(jnp.bfloat16)
        acc_ref[...] = jnp.zeros_like(acc_ref)
        groups = (occ_ref[x, y, z] + 31) // 32

        for group in range(1, slots // 32 + 1):

            @pl.when(groups == group)
            def _():
                rows = 32 * group
                lhs = jnp.concatenate([lhs_ref[0, :rows], lhs_ref[1, :rows]], axis=0)

                def column(i, carry):
                    sx = x + i // 3
                    sy = y + lax.rem(i, 3)
                    rhs = jnp.concatenate([base_ref[sx, sy, z + d] for d in range(3)], axis=1)
                    both = jnp.dot(lhs, rhs, preferred_element_type=jnp.float32)
                    inverse = lax.rsqrt(both[rows:])
                    weight = both[:rows] * (inverse * inverse * inverse)
                    sums = [0.0] * 4
                    for d in range(3):
                        part = weight[:, d * slots : (d + 1) * slots]
                        sums[3] = sums[3] + part
                        for k in range(3):
                            coord = place_ref[sx, sy, z + d, k : k + 1]
                            sums[k] = sums[k] + part * coord
                    for k in range(4):
                        acc_ref[k, :rows] += sums[k]
                    return carry

                lax.fori_loop(0, 9, column, 0)

        total = [jnp.sum(acc_ref[k], axis=1, keepdims=True) for k in range(4)]
        wide = jnp.where(
            lane == 0,
            total[0],
            jnp.where(lane == 1, total[1], jnp.where(lane == 2, total[2], total[3])),
        )
        flat = wide.T
        force = (place * flat[3:4] - flat[:8]) * (MU_SCALE * fix[3:4])
        emit(x, y, z, force)
        return carry

    lax.fori_loop(0, local[0] * local[1] * local[2], one_cell, 0)


def start_kernel(local, slots, occ_ref, fix_ref, pos_ref, mob_ref, speed_ref, peak_ref, *scratch):
    peak_ref[...] = jnp.zeros_like(peak_ref)

    def emit(x, y, z, force):
        mobility = mob_ref[x, y, pl.ds(z, 1)]
        speed = [mobility * force[k : k + 1] for k in range(3)]
        for k in range(3):
            speed_ref[k, x, y, pl.ds(z, 1)] = speed[k]
        square = speed[0] * speed[0] + speed[1] * speed[1] + speed[2] * speed[2]
        peak_ref[...] = jnp.maximum(peak_ref[...], square)

    sweep(local, slots, occ_ref, fix_ref, pos_ref, *scratch, emit)


def end_kernel(
    local, slots, occ_ref, step_ref, fix_ref, pos_ref, mob_ref, own_ref, speed_ref,
    moved_ref, end_ref, *scratch
):
    half = 0.5 * step_ref[0]

    def emit(x, y, z, force):
        mobility = mob_ref[x, y, pl.ds(z, 1)]
        for k in range(3):
            at = (k, x, y, pl.ds(z, 1))
            end_ref[at] = force[k : k + 1]
            moved_ref[at] = own_ref[at] + half * (speed_ref[at] + mobility * force[k : k + 1])

    sweep(local, slots, occ_ref, fix_ref, pos_ref, *scratch, emit)


def on_device(positions, line_vectors, burgers, mobility, occupancy):
    local, slots = mobility.shape[:3], mobility.shape[3]
    ext = tuple(n + 2 for n in local)
    smem = pl.BlockSpec(memory_space=pltpu.SMEM)
    vmem = pl.BlockSpec(memory_space=pltpu.VMEM)
    scratch = [
        pltpu.VMEM(ext + (128, slots), jnp.bfloat16),
        pltpu.VMEM(ext + (8, slots), jnp.float32),
        pltpu.VMEM((2, slots, 128), jnp.bfloat16),
        pltpu.VMEM((4, slots, slots), jnp.float32),
    ]
    params = pltpu.CompilerParams(vmem_limit_bytes=48 << 20)
    field = jax.ShapeDtypeStruct((3,) + mobility.shape, jnp.float32)

    lane = lax.broadcasted_iota(jnp.int32, mobility.shape, 3)
    live = (lane < occupancy[..., None]).astype(jnp.float32)
    zero = jnp.zeros_like(live)
    fix = jnp.stack(list(line_vectors) + [live] + list(burgers) + [zero], axis=3)
    rows = lambda p: jnp.stack(list(p) + [zero] * 5, axis=3)
    fix = extended(fix)
    speed, peaks = pl.pallas_call(
        functools.partial(start_kernel, local, slots),
        out_shape=(field, jax.ShapeDtypeStruct((1, slots), jnp.float32)),
        in_specs=[smem, vmem, vmem, vmem],
        out_specs=(vmem, vmem),
        scratch_shapes=scratch,
        compiler_params=params,
    )(occupancy, fix, extended(rows(positions)), mobility)
    peak = lax.pmax(jnp.max(peaks), AXES)
    step = STEP_LIMIT * lax.rsqrt(peak + 1e-12)
    predicted = positions + step * speed
    return tuple(
        pl.pallas_call(
            functools.partial(end_kernel, local, slots),
            out_shape=(field, field),
            in_specs=[smem, smem, vmem, vmem, vmem, vmem, vmem],
            out_specs=(vmem, vmem),
            scratch_shapes=scratch,
            compiler_params=params,
        )(occupancy, step[None], fix, extended(rows(predicted)), mobility, positions, speed)
    )


def solution(mesh):
    return jax.shard_map(
        on_device,
        mesh=mesh,
        in_specs=(
            P(None, "gx", "gy", "gz", None),
            P(None, "gx", "gy", "gz", None),
            P(None, "gx", "gy", "gz", None),
            P("gx", "gy", "gz", None),
            P("gx", "gy", "gz"),
        ),
        out_specs=(P(None, "gx", "gy", "gz", None), P(None, "gx", "gy", "gz", None)),
        check_vma=False,
    )
```

```python
import functools
import itertools

import jax
import jax.numpy as jnp
from jax import lax
from jax.experimental import pallas as pl
from jax.experimental.pallas import tpu as pltpu
from jax.sharding import PartitionSpec as P

CORE_SQUARED = 0.25
MU_SCALE = 0.05
CROSS_WEIGHT = 0.5
STEP_LIMIT = 0.1
AXES = ("gx", "gy", "gz")
K_ROWS = 72


def peers(shape):
    spans = [range(n) for n in shape]
    return [o for o in itertools.product(*spans) if any(o)]


def device_at(offset, shape):
    return tuple(
        lax.rem(lax.axis_index(a) + (o % n), n) for a, o, n in zip(AXES, offset, shape)
    )


def halo_messages(shape, local, block, padded):
    for shift in itertools.product((-1, 0, 1), repeat=3):
        if any(shift):
            take = tuple({-1: pl.ds(0, 1), 0: pl.ds(0, n), 1: pl.ds(n - 1, 1)}[s] for s, n in zip(shift, local))
            put = tuple({-1: pl.ds(n + 1, 1), 0: pl.ds(1, n), 1: pl.ds(0, 1)}[s] for s, n in zip(shift, local))
            yield device_at(shift, shape), block.at[take], padded.at[put]


def exchange(shape, local, blocks, padded, extra, greet, send_sem, recv_sem, own_sem):
    barrier = pltpu.get_barrier_semaphore()
    for offset in greet:
        pl.semaphore_signal(
            barrier, inc=1, device_id=device_at(offset, shape), device_id_type=pl.DeviceIdType.MESH
        )
    inner = tuple(pl.ds(1, n) for n in local)
    own = [
        pltpu.make_async_copy(b, p.at[inner], own_sem.at[i])
        for i, (b, p) in enumerate(zip(blocks, padded))
    ]
    for copy in own:
        copy.start()
    messages = list(extra)
    for b, p in zip(blocks, padded):
        messages += list(halo_messages(shape, local, b, p))
    pl.semaphore_wait(barrier, len(greet))
    copies = [
        pltpu.make_async_remote_copy(
            src_ref=source,
            dst_ref=target,
            send_sem=send_sem.at[i],
            recv_sem=recv_sem.at[i],
            device_id=device,
            device_id_type=pl.DeviceIdType.MESH,
        )
        for i, (device, source, target) in enumerate(messages)
    ]
    for copy in copies:
        copy.start()
    for copy in copies + own:
        copy.wait()


def fixed_halo_kernel(shape, local, fix_ref, rest_ref, fix_out, rest_out, *sems):
    near = [s for s in itertools.product((-1, 0, 1), repeat=3) if any(s)]
    exchange(shape, local, (fix_ref, rest_ref), (fix_out, rest_out), [], near, *sems)


def speed_halo_kernel(shape, local, speed_ref, peak_ref, speed_out, peaks_out, *sems):
    others = peers(shape)
    extra = [
        (device_at(o, shape), peak_ref, peaks_out.at[i]) for i, o in enumerate(others)
    ]
    exchange(shape, local, (speed_ref,), (speed_out,), extra, others, *sems)


def halo_call(kernel, out_shape, messages, collective, *args):
    vmem = pl.BlockSpec(memory_space=pltpu.VMEM)
    return pl.pallas_call(
        kernel,
        out_shape=out_shape,
        in_specs=[vmem] * len(args),
        out_specs=tuple(vmem for _ in out_shape),
        scratch_shapes=[
            pltpu.SemaphoreType.DMA((messages,)),
            pltpu.SemaphoreType.DMA((messages,)),
            pltpu.SemaphoreType.DMA((2,)),
        ],
        compiler_params=pltpu.CompilerParams(collective_id=collective, has_side_effects=True),
    )(*args)


def split(value, parts):
    terms = []
    for _ in range(parts):
        term = value.astype(jnp.bfloat16).astype(jnp.float32)
        terms.append(term)
        value = value - term
    return terms


def offsets(row, index, local):
    corner = [i.astype(jnp.float32) - (1.0 + n / 2) for i, n in zip(index, local)]
    return jnp.where(row == 0, corner[0], jnp.where(row == 1, corner[1], corner[2]))


def source_rows(fix, place, row):
    live = fix[3:4]
    turned = pltpu.roll(fix, 4, 0)
    keep = jnp.where(row < 3, live, 0.0)
    lines, burgers = fix * keep, turned * keep
    high, low = [], []
    for a in range(3):
        form = fix[4 + a : 5 + a] * lines - CROSS_WEIGHT * fix[a : a + 1] * burgers
        first, second = split(form, 2)
        high.append(first)
        low.append(second)
    square = jnp.sum(place * place, axis=0, keepdims=True) + CORE_SQUARED
    vec = jnp.where(row < 3, place, jnp.where(row == 3, square, jnp.where(row == 4, 1.0, 0.0)))
    h, m, l = split(vec, 3)
    zero = jnp.zeros_like(h)
    return jnp.concatenate(high + low + high + [h, m, h, m, l, h, zero], axis=0)


def target_rows(fix, place, row):
    high, low = [], []
    for a in range(3):
        first, second = split(fix[4 + a : 5 + a] * fix, 2)
        high.append(first)
        low.append(second)
    square = jnp.sum(place * place, axis=0, keepdims=True)
    vec = jnp.where(
        row < 3, -2.0 * place, jnp.where(row == 3, 1.0, jnp.where(row == 4, square, 0.0))
    )
    h, m, l = split(vec, 3)
    zero = jnp.zeros_like(h)
    return jnp.concatenate(high + high + low + [h, h, m, m, h, l, zero], axis=0)


def sweep(local, slots, occ_ref, fix_ref, spot, base_ref, place_ref, lhs_ref, acc_ref, emit):
    ext = tuple(n + 2 for n in local)
    row = lax.broadcasted_iota(jnp.int32, (8, slots), 0)

    def prepare(c, carry):
        z = lax.rem(c, ext[2])
        y = lax.rem(c // ext[2], ext[1])
        x = c // (ext[2] * ext[1])
        place = jnp.where(row < 3, spot(x, y, z) + offsets(row, (x, y, z), local), 0.0)
        place_ref[x, y, z] = place
        base_ref[x, y, z] = source_rows(fix_ref[x, y, z], place, row).astype(jnp.bfloat16)
        return carry

    lax.fori_loop(0, ext[0] * ext[1] * ext[2], prepare, 0)

    def one_cell(c, carry):
        z = lax.rem(c, local[2])
        y = lax.rem(c // local[2], local[1])
        x = c // (local[2] * local[1])
        fix = fix_ref[x + 1, y + 1, z + 1]
        place = place_ref[x + 1, y + 1, z + 1]
        turned = target_rows(fix, place, row).T
        lane = lax.broadcasted_iota(jnp.int32, turned.shape, 1)
        lhs_ref[0] = jnp.where(lane < K_ROWS, turned, 0.0).astype(jnp.bfloat16)
        lhs_ref[1] = jnp.where(lane < K_ROWS, 0.0, turned).astype(jnp.bfloat16)
        acc_ref[...] = jnp.zeros_like(acc_ref)
        groups = (occ_ref[x, y, z] + 31) // 32

        for group in range(1, slots // 32 + 1):

            @pl.when(groups == group)
            def _():
                rows = 32 * group
                lhs = jnp.concatenate([lhs_ref[0, :rows], lhs_ref[1, :rows]], axis=0)

                for i, j in itertools.product(range(3), repeat=2):
                    near = [(x + i, y + j, z + d) for d in range(3)]
                    rhs = jnp.concatenate([base_ref[at] for at in near], axis=1)
                    both = jnp.dot(lhs, rhs, preferred_element_type=jnp.float32)
                    inverse = lax.rsqrt(both[rows:])
                    weight = both[:rows] * (inverse * inverse * inverse)
                    sums = [0.0] * 4
                    for d, at in enumerate(near):
                        part = weight[:, d * slots : (d + 1) * slots]
                        sums[3] = sums[3] + part
                        for k in range(3):
                            sums[k] = sums[k] + part * place_ref[at + (pl.ds(k, 1),)]
                    for k in range(4):
                        acc_ref[k, :rows] += sums[k]

        total = [jnp.sum(acc_ref[k], axis=1, keepdims=True) for k in range(4)]
        wide = jnp.where(
            lane == 0,
            total[0],
            jnp.where(lane == 1, total[1], jnp.where(lane == 2, total[2], total[3])),
        )
        flat = wide.T
        force = (place * flat[3:4] - flat[:8]) * (MU_SCALE * fix[3:4])
        emit(x, y, z, force)
        return carry

    lax.fori_loop(0, local[0] * local[1] * local[2], one_cell, 0)


def stacked(parts):
    fill = jnp.zeros((8 - sum(p.shape[0] for p in parts),) + parts[0].shape[1:], jnp.float32)
    return jnp.concatenate(list(parts) + [fill], axis=0)


def start_kernel(local, slots, occ_ref, fix_ref, rest_ref, mob_ref, speed_ref, peak_ref, *scratch):
    peak_ref[...] = jnp.zeros_like(peak_ref)

    def spot(x, y, z):
        return stacked([fix_ref[x, y, z, 7:8], rest_ref[x, y, z]])

    def emit(x, y, z, force):
        speed = mob_ref[x, y, pl.ds(z, 1)] * force
        speed_ref[x, y, z] = speed[:4]
        square = speed[0:1] * speed[0:1] + speed[1:2] * speed[1:2] + speed[2:3] * speed[2:3]
        peak_ref[...] = jnp.maximum(peak_ref[...], square)

    sweep(local, slots, occ_ref, fix_ref, spot, *scratch, emit)


def end_kernel(
    local, slots, occ_ref, fix_ref, rest_ref, mob_ref, own_ref, speed_ref, peak_ref, peaks_ref,
    moved_ref, end_ref, *scratch
):
    peak = jnp.maximum(peak_ref[...], jnp.max(peaks_ref[...], axis=0))
    peak = jnp.max(peak, axis=1, keepdims=True)
    step = STEP_LIMIT * lax.rsqrt(peak + 1e-12)

    def spot(x, y, z):
        place = stacked([fix_ref[x, y, z, 7:8], rest_ref[x, y, z]])
        return place + step * stacked([speed_ref[x, y, z]])

    def emit(x, y, z, force):
        mobility = mob_ref[x, y, pl.ds(z, 1)]
        speed = speed_ref[x + 1, y + 1, z + 1]
        for k in range(3):
            at = (k, x, y, pl.ds(z, 1))
            end_ref[at] = force[k : k + 1]
            moved_ref[at] = own_ref[at] + (0.5 * step) * (
                speed[k : k + 1] + mobility * force[k : k + 1]
            )

    sweep(local, slots, occ_ref, fix_ref, spot, *scratch, emit)


def on_device(shape, positions, line_vectors, burgers, mobility, occupancy):
    local, slots = mobility.shape[:3], mobility.shape[3]
    ext = tuple(n + 2 for n in local)
    smem = pl.BlockSpec(memory_space=pltpu.SMEM)
    vmem = pl.BlockSpec(memory_space=pltpu.VMEM)
    scratch = [
        pltpu.VMEM(ext + (128, slots), jnp.bfloat16),
        pltpu.VMEM(ext + (8, slots), jnp.float32),
        pltpu.VMEM((2, slots, 128), jnp.bfloat16),
        pltpu.VMEM((4, slots, slots), jnp.float32),
    ]
    params = pltpu.CompilerParams(vmem_limit_bytes=48 << 20)
    rows = lambda lead, n: jax.ShapeDtypeStruct(lead + (n, slots), jnp.float32)
    field = jax.ShapeDtypeStruct((3,) + mobility.shape, jnp.float32)
    others = len(peers(shape))

    lane = lax.broadcasted_iota(jnp.int32, mobility.shape, 3)
    live = (lane < occupancy[..., None]).astype(jnp.float32)
    fix = jnp.stack(list(line_vectors) + [live] + list(burgers) + [positions[0]], axis=3)
    rest = jnp.stack(list(positions[1:]), axis=3)
    fix, rest = halo_call(
        functools.partial(fixed_halo_kernel, shape, local),
        (rows(ext, 8), rows(ext, 2)),
        52,
        0,
        fix,
        rest,
    )
    speed, peak = pl.pallas_call(
        functools.partial(start_kernel, local, slots),
        out_shape=(rows(local, 4), rows((), 1)),
        in_specs=[smem, vmem, vmem, vmem],
        out_specs=(vmem, vmem),
        scratch_shapes=scratch,
        compiler_params=params,
    )(occupancy, fix, rest, mobility)
    speed, peaks = halo_call(
        functools.partial(speed_halo_kernel, shape, local),
        (rows(ext, 4), rows((others,), 1)),
        26 + others,
        1,
        speed,
        peak,
    )
    return tuple(
        pl.pallas_call(
            functools.partial(end_kernel, local, slots),
            out_shape=(field, field),
            in_specs=[smem] + [vmem] * 7,
            out_specs=(vmem, vmem),
            scratch_shapes=scratch,
            compiler_params=params,
        )(occupancy, fix, rest, mobility, positions, speed, peak, peaks)
    )


def solution(mesh):
    return jax.shard_map(
        functools.partial(on_device, tuple(mesh.shape[a] for a in AXES)),
        mesh=mesh,
        in_specs=(
            P(None, "gx", "gy", "gz", None),
            P(None, "gx", "gy", "gz", None),
            P(None, "gx", "gy", "gz", None),
            P("gx", "gy", "gz", None),
            P("gx", "gy", "gz"),
        ),
        out_specs=(P(None, "gx", "gy", "gz", None), P(None, "gx", "gy", "gz", None)),
        check_vma=False,
    )
```

```python
import functools
import itertools

import jax
import jax.numpy as jnp
from jax import lax
from jax.experimental import pallas as pl
from jax.experimental.pallas import tpu as pltpu
from jax.sharding import PartitionSpec as P

CORE_SQUARED = 0.25
MU_SCALE = 0.05
CROSS_WEIGHT = 0.5
STEP_LIMIT = 0.1
AXES = ("gx", "gy", "gz")
K_ROWS = 72


def peers(shape):
    spans = [range(n) for n in shape]
    return [o for o in itertools.product(*spans) if any(o)]


def device_at(offset, shape):
    return tuple(
        lax.rem(lax.axis_index(a) + (o % n), n) for a, o, n in zip(AXES, offset, shape)
    )


def halo_messages(shape, local, block, padded):
    for shift in itertools.product((-1, 0, 1), repeat=3):
        if any(shift):
            take = tuple({-1: pl.ds(0, 1), 0: pl.ds(0, n), 1: pl.ds(n - 1, 1)}[s] for s, n in zip(shift, local))
            put = tuple({-1: pl.ds(n + 1, 1), 0: pl.ds(1, n), 1: pl.ds(0, 1)}[s] for s, n in zip(shift, local))
            yield device_at(shift, shape), block.at[take], padded.at[put]


def exchange(shape, local, blocks, padded, extra, greet, send_sem, recv_sem, own_sem):
    barrier = pltpu.get_barrier_semaphore()
    for offset in greet:
        pl.semaphore_signal(
            barrier, inc=1, device_id=device_at(offset, shape), device_id_type=pl.DeviceIdType.MESH
        )
    inner = tuple(pl.ds(1, n) for n in local)
    own = [
        pltpu.make_async_copy(b, p.at[inner], own_sem.at[i])
        for i, (b, p) in enumerate(zip(blocks, padded))
    ]
    for copy in own:
        copy.start()
    messages = list(extra)
    for b, p in zip(blocks, padded):
        messages += list(halo_messages(shape, local, b, p))
    pl.semaphore_wait(barrier, len(greet))
    copies = [
        pltpu.make_async_remote_copy(
            src_ref=source,
            dst_ref=target,
            send_sem=send_sem.at[i],
            recv_sem=recv_sem.at[i],
            device_id=device,
            device_id_type=pl.DeviceIdType.MESH,
        )
        for i, (device, source, target) in enumerate(messages)
    ]
    for copy in copies:
        copy.start()
    for copy in copies + own:
        copy.wait()


def fixed_halo_kernel(shape, local, fix_ref, rest_ref, fix_out, rest_out, *sems):
    near = [s for s in itertools.product((-1, 0, 1), repeat=3) if any(s)]
    exchange(shape, local, (fix_ref, rest_ref), (fix_out, rest_out), [], near, *sems)


def speed_halo_kernel(shape, local, speed_ref, peak_ref, speed_out, peaks_out, *sems):
    others = peers(shape)
    extra = [
        (device_at(o, shape), peak_ref, peaks_out.at[i]) for i, o in enumerate(others)
    ]
    exchange(shape, local, (speed_ref,), (speed_out,), extra, others, *sems)


def halo_call(kernel, out_shape, messages, collective, *args):
    vmem = pl.BlockSpec(memory_space=pltpu.VMEM)
    return pl.pallas_call(
        kernel,
        out_shape=out_shape,
        in_specs=[vmem] * len(args),
        out_specs=tuple(vmem for _ in out_shape),
        scratch_shapes=[
            pltpu.SemaphoreType.DMA((messages,)),
            pltpu.SemaphoreType.DMA((messages,)),
            pltpu.SemaphoreType.DMA((2,)),
        ],
        compiler_params=pltpu.CompilerParams(collective_id=collective, has_side_effects=True, vmem_limit_bytes=8 << 20),
    )(*args)


def split(value, parts):
    terms = []
    for _ in range(parts):
        term = value.astype(jnp.bfloat16).astype(jnp.float32)
        terms.append(term)
        value = value - term
    return terms


def offsets(row, index, local):
    corner = [i.astype(jnp.float32) - (1.0 + n / 2) for i, n in zip(index, local)]
    return jnp.where(row == 0, corner[0], jnp.where(row == 1, corner[1], corner[2]))


def source_rows(fix, place, row):
    live = fix[3:4]
    turned = pltpu.roll(fix, 4, 0)
    keep = jnp.where(row < 3, live, 0.0)
    lines, burgers = fix * keep, turned * keep
    high, low = [], []
    for a in range(3):
        form = fix[4 + a : 5 + a] * lines - CROSS_WEIGHT * fix[a : a + 1] * burgers
        first, second = split(form, 2)
        high.append(first)
        low.append(second)
    square = jnp.sum(place * place, axis=0, keepdims=True) + CORE_SQUARED
    vec = jnp.where(row < 3, place, jnp.where(row == 3, square, jnp.where(row == 4, 1.0, 0.0)))
    h, m, l = split(vec, 3)
    zero = jnp.zeros_like(h)
    return jnp.concatenate(high + low + high + [h, m, h, m, l, h, zero], axis=0)


def target_rows(fix, place, row):
    high, low = [], []
    for a in range(3):
        first, second = split(fix[4 + a : 5 + a] * fix, 2)
        high.append(first)
        low.append(second)
    square = jnp.sum(place * place, axis=0, keepdims=True)
    vec = jnp.where(
        row < 3, -2.0 * place, jnp.where(row == 3, 1.0, jnp.where(row == 4, square, 0.0))
    )
    h, m, l = split(vec, 3)
    zero = jnp.zeros_like(h)
    return jnp.concatenate(high + high + low + [h, h, m, m, h, l, zero], axis=0)


def sweep(local, slots, occ_ref, fix_ref, spot, base_ref, place_ref, lhs_ref, acc_ref, emit):
    ext = tuple(n + 2 for n in local)
    row = lax.broadcasted_iota(jnp.int32, (8, slots), 0)

    def prepare(c, carry):
        x, y = c // ext[1], lax.rem(c, ext[1])
        for z in range(ext[2]):
            corner = offsets(row, (x, y, jnp.int32(z)), local)
            place = jnp.where(row < 3, spot(x, y, z) + corner, 0.0)
            place_ref[x, y, z] = place
            base_ref[x, y, z] = source_rows(fix_ref[x, y, z], place, row).astype(jnp.bfloat16)
        return carry

    lax.fori_loop(0, ext[0] * ext[1], prepare, 0)

    def one_cell(c, carry):
        z = lax.rem(c, local[2])
        y = lax.rem(c // local[2], local[1])
        x = c // (local[2] * local[1])
        fix = fix_ref[x + 1, y + 1, z + 1]
        place = place_ref[x + 1, y + 1, z + 1]
        turned = target_rows(fix, place, row).T
        lane = lax.broadcasted_iota(jnp.int32, turned.shape, 1)
        lhs_ref[0] = jnp.where(lane < K_ROWS, turned, 0.0).astype(jnp.bfloat16)
        lhs_ref[1] = jnp.where(lane < K_ROWS, 0.0, turned).astype(jnp.bfloat16)
        acc_ref[...] = jnp.zeros_like(acc_ref)
        groups = (occ_ref[x, y, z] + 15) // 16

        for group in range(1, slots // 16 + 1):

            @pl.when(groups == group)
            def _():
                rows = 16 * group
                lhs = jnp.concatenate([lhs_ref[0, :rows], lhs_ref[1, :rows]], axis=0)

                for i, j in itertools.product(range(3), repeat=2):
                    near = [(x + i, y + j, z + d) for d in range(3)]
                    rhs = jnp.concatenate([base_ref[at] for at in near], axis=1)
                    both = jnp.dot(lhs, rhs, preferred_element_type=jnp.float32)
                    inverse = lax.rsqrt(both[rows:])
                    weight = both[:rows] * (inverse * inverse * inverse)
                    sums = [0.0] * 4
                    for d, at in enumerate(near):
                        part = weight[:, d * slots : (d + 1) * slots]
                        sums[3] = sums[3] + part
                        for k in range(3):
                            sums[k] = sums[k] + part * place_ref[at + (pl.ds(k, 1),)]
                    for k in range(4):
                        acc_ref[k, :rows] += sums[k]

        total = [jnp.sum(acc_ref[k], axis=1, keepdims=True) for k in range(4)]
        wide = jnp.where(
            lane == 0,
            total[0],
            jnp.where(lane == 1, total[1], jnp.where(lane == 2, total[2], total[3])),
        )
        flat = wide.T
        force = (place * flat[3:4] - flat[:8]) * (MU_SCALE * fix[3:4])
        emit(x, y, z, force)
        return carry

    lax.fori_loop(0, local[0] * local[1] * local[2], one_cell, 0)


def stacked(parts):
    fill = jnp.zeros((8 - sum(p.shape[0] for p in parts),) + parts[0].shape[1:], jnp.float32)
    return jnp.concatenate(list(parts) + [fill], axis=0)


def start_kernel(local, slots, occ_ref, fix_ref, rest_ref, mob_ref, speed_ref, peak_ref, *scratch):
    peak_ref[...] = jnp.zeros_like(peak_ref)

    def spot(x, y, z):
        return stacked([fix_ref[x, y, z, 7:8], rest_ref[x, y, z]])

    def emit(x, y, z, force):
        speed = mob_ref[x, y, pl.ds(z, 1)] * force
        speed_ref[x, y, z] = speed[:4]
        square = speed[0:1] * speed[0:1] + speed[1:2] * speed[1:2] + speed[2:3] * speed[2:3]
        peak_ref[...] = jnp.maximum(peak_ref[...], square)

    sweep(local, slots, occ_ref, fix_ref, spot, *scratch, emit)


def end_kernel(
    local, slots, occ_ref, fix_ref, rest_ref, mob_ref, own_ref, speed_ref, peak_ref, peaks_ref,
    moved_ref, end_ref, *scratch
):
    peak = jnp.maximum(peak_ref[...], jnp.max(peaks_ref[...], axis=0))
    peak = jnp.max(peak, axis=1, keepdims=True)
    step = STEP_LIMIT * lax.rsqrt(peak + 1e-12)

    def spot(x, y, z):
        place = stacked([fix_ref[x, y, z, 7:8], rest_ref[x, y, z]])
        return place + step * stacked([speed_ref[x, y, z]])

    def emit(x, y, z, force):
        mobility = mob_ref[x, y, pl.ds(z, 1)]
        speed = speed_ref[x + 1, y + 1, z + 1]
        for k in range(3):
            at = (k, x, y, pl.ds(z, 1))
            end_ref[at] = force[k : k + 1]
            moved_ref[at] = own_ref[at] + (0.5 * step) * (
                speed[k : k + 1] + mobility * force[k : k + 1]
            )

    sweep(local, slots, occ_ref, fix_ref, spot, *scratch, emit)


def on_device(shape, positions, line_vectors, burgers, mobility, occupancy):
    local, slots = mobility.shape[:3], mobility.shape[3]
    ext = tuple(n + 2 for n in local)
    smem = pl.BlockSpec(memory_space=pltpu.SMEM)
    vmem = pl.BlockSpec(memory_space=pltpu.VMEM)
    scratch = [
        pltpu.VMEM(ext + (128, slots), jnp.bfloat16),
        pltpu.VMEM(ext + (8, slots), jnp.float32),
        pltpu.VMEM((2, slots, 128), jnp.bfloat16),
        pltpu.VMEM((4, slots, slots), jnp.float32),
    ]
    params = pltpu.CompilerParams(vmem_limit_bytes=16 << 20)
    rows = lambda lead, n: jax.ShapeDtypeStruct(lead + (n, slots), jnp.float32)
    field = jax.ShapeDtypeStruct((3,) + mobility.shape, jnp.float32)
    others = len(peers(shape))

    lane = lax.broadcasted_iota(jnp.int32, mobility.shape, 3)
    live = (lane < occupancy[..., None]).astype(jnp.float32)
    fix = jnp.stack(list(line_vectors) + [live] + list(burgers) + [positions[0]], axis=3)
    rest = jnp.stack(list(positions[1:]), axis=3)
    fix, rest = halo_call(
        functools.partial(fixed_halo_kernel, shape, local),
        (rows(ext, 8), rows(ext, 2)),
        52,
        0,
        fix,
        rest,
    )
    speed, peak = pl.pallas_call(
        functools.partial(start_kernel, local, slots),
        out_shape=(rows(local, 4), rows((), 1)),
        in_specs=[smem, vmem, vmem, vmem],
        out_specs=(vmem, vmem),
        scratch_shapes=scratch,
        compiler_params=params,
    )(occupancy, fix, rest, mobility)
    speed, peaks = halo_call(
        functools.partial(speed_halo_kernel, shape, local),
        (rows(ext, 4), rows((others,), 1)),
        26 + others,
        1,
        speed,
        peak,
    )
    return tuple(
        pl.pallas_call(
            functools.partial(end_kernel, local, slots),
            out_shape=(field, field),
            in_specs=[smem] + [vmem] * 7,
            out_specs=(vmem, vmem),
            scratch_shapes=scratch,
            compiler_params=params,
        )(occupancy, fix, rest, mobility, positions, speed, peak, peaks)
    )


def solution(mesh):
    return jax.shard_map(
        functools.partial(on_device, tuple(mesh.shape[a] for a in AXES)),
        mesh=mesh,
        in_specs=(
            P(None, "gx", "gy", "gz", None),
            P(None, "gx", "gy", "gz", None),
            P(None, "gx", "gy", "gz", None),
            P("gx", "gy", "gz", None),
            P("gx", "gy", "gz"),
        ),
        out_specs=(P(None, "gx", "gy", "gz", None), P(None, "gx", "gy", "gz", None)),
        check_vma=False,
    )
```
